8 devices in a mesh: dp: 1 (over z), tp: 8 (over x, y, core).
Axes of the slice: x: 2, y: 2, z: 1, core: 2. Of those that a mesh axis runs over, the one named last changes fastest.
Arguments:
- x: bfloat16 [2048, 7168], P('dp')
- w_gate: bfloat16 [7168, 18432], P(None, 'tp')
- w_up: bfloat16 [7168, 18432], P(None, 'tp')
- w_down: bfloat16 [18432, 7168], P('tp')
Outputs:
- output: bfloat16 [2048, 7168], P('dp')
All inputs are finite; a program needn't handle non-finite values.
Results may differ from the reference program's by a relative error of at most 0.016.
Values are sent between devices in bfloat16 or wider.
A program may use at most 2 GiB of HBM per device.

```python
import jax
import jax.numpy as jnp

ROWS = 2048
D = 7168
FF = 18432


def setup_inputs(seed: int = 0, part: int = 0) -> dict:
    kx, kg, ku, kd = jax.random.split(jax.random.key(seed), 4)
    drawn = {
        "x": jax.random.normal(jax.random.fold_in(kx, part), (ROWS, D), jnp.float32),
        "w_gate": jax.random.normal(kg, (D, FF), jnp.float32) * D**-0.5,
        "w_up": jax.random.normal(ku, (D, FF), jnp.float32) * D**-0.5,
        "w_down": jax.random.normal(kd, (FF, D), jnp.float32) * FF**-0.5,
    }
    return {k: v.astype(jnp.bfloat16) for k, v in drawn.items()}


def reference(x, w_gate, w_up, w_down):
    gate = jnp.dot(x, w_gate, preferred_element_type=jnp.float32)
    up = jnp.dot(x, w_up, preferred_element_type=jnp.float32)
    hidden = (jax.nn.silu(gate) * up).astype(jnp.bfloat16)
    return jnp.dot(hidden, w_down, preferred_element_type=jnp.float32).astype(jnp.bfloat16)
```

```python
import functools

import jax
import jax.numpy as jnp
from jax import lax
from jax.experimental import pallas as pl
from jax.experimental.pallas import tpu as pltpu
from jax.sharding import PartitionSpec as P

MESH = pl.DeviceIdType.MESH
BF16, F32 = jnp.bfloat16, jnp.float32
M = 256
HALF, QUARTER, EIGHTH = M // 2, M // 4, M // 8
TH = 256
W = 1024


def kernel(
    n_chunks, n_gu, n_dn,
    x_hbm, wg_hbm, wu_hbm, wd_hbm, y_hbm,
    xbuf, wbuf, acc, hbuf, wdbuf, keep, sp, rp, k1, s1, r1, k2, s2, r2, fin,
    x_sem, w_sem, wd_sem, p_send, p_recv, a_send, a_recv, b_send, b_recv,
    loc_sem, g1_send, g1_recv, g2_send, g2_recv, g3_send, g3_recv, q_send, q_recv, credit,
):
    me = lax.axis_index("tp")
    dx, dy, dc = me // 4, (me // 2) % 2, me % 2
    sib = me + 1 - 2 * dc
    depth = x_hbm.shape[1]
    kh = depth // 2
    n_tiles = n_chunks * n_gu
    n_units = n_chunks * n_dn

    def remote(src, dst, send, recv, dev):
        return pltpu.make_async_remote_copy(
            src_ref=src, dst_ref=dst, send_sem=send, recv_sem=recv, device_id={"tp": dev}, device_id_type=MESH
        )

    def w_copies(t, part):
        col = pl.multiple_of((t % n_gu) * TH, TH)
        rows = pl.ds(part * kh, kh)
        slot = t % 2
        return [
            pltpu.make_async_copy(
                src.at[rows, pl.ds(col, TH)], wbuf.at[slot, rows, pl.ds(TH * n, TH)], w_sem.at[slot, part, n]
            )
            for n, src in enumerate((wg_hbm, wu_hbm))
        ]

    def x_copies(k):
        own = pl.multiple_of(k * M + dc * HALF, HALF)
        other = pl.multiple_of(k * M + (1 - dc) * HALF, HALF)
        return [
            pltpu.make_async_copy(x_hbm.at[pl.ds(own, HALF)], xbuf.at[pl.ds(0, HALF)], x_sem.at[0]),
            pltpu.make_async_copy(x_hbm.at[pl.ds(other, HALF)], xbuf.at[pl.ds(HALF, HALF)], x_sem.at[1]),
        ]

    def wd_copy(j):
        return pltpu.make_async_copy(
            wd_hbm.at[:, pl.ds(pl.multiple_of(j * W, W), W)], wdbuf.at[j], wd_sem.at[j]
        )

    def pair_copy(j):
        return remote(sp.at[j], rp.at[j], p_send.at[j], p_recv.at[j], sib)

    def place(u):
        e = u % 2
        xa, ya = dx + (1 - e) * (1 - 2 * dx), dy + e * (1 - 2 * dy)
        xb, yb = dx + e * (1 - 2 * dx), dy + (1 - e) * (1 - 2 * dy)
        p, r = dx * (1 - e) + dy * e, dx * e + dy * (1 - e)
        return 4 * xa + 2 * ya + dc, 4 * xb + 2 * yb + dc, p, r

    def block(u, p, r):
        row = pl.multiple_of((u // n_dn) * M + dc * HALF + p * QUARTER + r * EIGHTH, EIGHTH)
        return y_hbm.at[pl.ds(row, EIGHTH), pl.ds(pl.multiple_of((u % n_dn) * W, W), W)]

    def half_block(u):
        row = pl.multiple_of((u // n_dn) * M + dc * HALF, HALF)
        return y_hbm.at[pl.ds(row, HALF), pl.ds(pl.multiple_of((u % n_dn) * W, W), W)]

    def a_copy(u):
        a, _, _, _ = place(u)
        s = u % 4
        return remote(s1.at[s], r1.at[s], a_send.at[s], a_recv.at[s], a)

    def b_copy(u):
        _, b, _, _ = place(u)
        s = u % 4
        return remote(s2.at[s], r2.at[s], b_send.at[s], b_recv.at[s], b)

    def loc_copy(u):
        _, _, p, r = place(u)
        return pltpu.make_async_copy(fin.at[u % 4], block(u, p, r), loc_sem.at[u % 4])

    def g1_copy(u):
        _, b, p, r = place(u)
        return remote(fin.at[u % 4], block(u, p, r), g1_send.at[u % 4], g1_recv.at[u % 4], b)

    def g2_copy(u):
        a, _, p, r = place(u)
        return remote(fin.at[u % 4], block(u, p, r), g2_send.at[u % 4], g2_recv.at[u % 8], a)

    def g3_copy(u):
        a, _, p, r = place(u)
        blk = block(u, p, 1 - r)
        return remote(blk, blk, g3_send.at[u % 4], g3_recv.at[u % 8], a)

    def q_copy(u):
        blk = half_block(u)
        return remote(blk, blk, q_send, q_recv, sib)

    def tick(n):
        u5, u4, u3, u2, u1 = n - 8, n - 6, n - 4, n - 2, n

        @pl.when(u5 >= 0)
        def _():
            loc_copy(u5).wait()
            g1_copy(u5).wait_send()
            g2_copy(u5).wait()
            g3_copy(u5).wait()
            q_copy(u5).start()

        @pl.when((u4 >= 0) & (u4 < n_units))
        def _():
            g1_copy(u4).wait_recv()
            g3_copy(u4).start()

        @pl.when((u3 >= 0) & (u3 < n_units))
        def _():
            b_copy(u3).wait()
            s = u3 % 4
            fin[s] = (k2[s] + r2[s].astype(F32)).astype(BF16)
            g1_copy(u3).start()
            g2_copy(u3).start()
            loc_copy(u3).start()

        @pl.when((u2 >= 0) & (u2 < n_units))
        def _():
            a_copy(u2).wait()
            s = u2 % 4
            _, _, _, r = place(u2)
            mine = pl.ds(pl.multiple_of(r * EIGHTH, EIGHTH), EIGHTH)
            theirs = pl.ds(pl.multiple_of((1 - r) * EIGHTH, EIGHTH), EIGHTH)
            s2[s] = (k1[s, theirs] + r1[s, theirs].astype(F32)).astype(BF16)
            b_copy(u2).start()
            k2[s] = k1[s, mine] + r1[s, mine].astype(F32)

        @pl.when(u1 < n_units)
        def _():
            j = u1 % n_dn
            pair_copy(j).wait()
            s = u1 % 4
            _, _, p, _ = place(u1)
            mine = pl.ds(pl.multiple_of(p * QUARTER, QUARTER), QUARTER)
            theirs = pl.ds(pl.multiple_of((1 - p) * QUARTER, QUARTER), QUARTER)
            s1[s] = (keep[j, theirs] + rp[j, theirs].astype(F32)).astype(BF16)
            a_copy(u1).start()
            k1[s] = keep[j, mine] + rp[j, mine].astype(F32)

    for c in x_copies(0):
        c.start()
    for t in range(2):
        for part in range(2):
            for c in w_copies(t, part):
                c.start()

    barrier = pltpu.get_barrier_semaphore()
    partners = (sib, 4 * (1 - dx) + 2 * dy + dc, 4 * dx + 2 * (1 - dy) + dc)
    for dev in partners:
        pl.semaphore_signal(barrier, inc=1, device_id={"tp": dev}, device_id_type=MESH)
    pl.semaphore_wait(barrier, 3)

    def chunk(k, _):
        for c in x_copies(k):
            c.wait()

        def gate_up(i, _):
            t = k * n_gu + i
            slot = t % 2

            @pl.when((k > 0) & (i % 2 == 0))
            def _():
                tick((k - 1) * n_dn + 2 + i // 2)

            for c in w_copies(t, 0):
                c.wait()
            acc[...] = jnp.dot(xbuf[:, :kh], wbuf[slot, :kh], preferred_element_type=F32)

            @pl.when(t + 2 < n_tiles)
            def _():
                for c in w_copies(t + 2, 0):
                    c.start()

            for c in w_copies(t, 1):
                c.wait()
            gu = acc[...] + jnp.dot(xbuf[:, kh:], wbuf[slot, kh:], preferred_element_type=F32)
            g, up = gu[:, :TH], gu[:, TH:]
            hbuf[:, pl.ds(pl.multiple_of(i * TH, TH), TH)] = (g * jax.nn.sigmoid(g) * up).astype(BF16)

            @pl.when(t + 2 < n_tiles)
            def _():
                for c in w_copies(t + 2, 1):
                    c.start()

            @pl.when((k == 0) & (i >= n_gu - 2))
            def _():
                wd_copy(i - (n_gu - 2)).start()

            return 0

        lax.fori_loop(0, n_gu, gate_up, 0)

        @pl.when(k + 1 < n_chunks)
        def _():
            for c in x_copies(k + 1):
                c.start()

        @pl.when(k > 0)
        def _():
            pl.semaphore_signal(credit, inc=1, device_id={"tp": sib}, device_id_type=MESH)
            pl.semaphore_wait(credit, 1)

        def down(j, _):
            @pl.when(k == 0)
            def _():
                wd_copy(j).wait()

                @pl.when(j + 2 < n_dn)
                def _():
                    wd_copy(j + 2).start()

            term = jnp.dot(hbuf[...], wdbuf[j], preferred_element_type=F32)
            sp[j] = term[HALF:].astype(BF16)
            keep[j] = term[:HALF]
            pair_copy(j).start()

            @pl.when((j == 2) | (j == 5))
            def _():
                tick(k * n_dn + (j - 2) // 3)

            return 0

        lax.fori_loop(0, n_dn, down, 0)
        return 0

    lax.fori_loop(0, n_chunks, chunk, 0)

    def last(n, _):
        tick(n)
        return 0

    lax.fori_loop((n_chunks - 1) * n_dn + 2, n_units + 8, last, 0)
    half_y = y_hbm.at[pl.ds(0, y_hbm.shape[0] // 2)]
    done = remote(half_y, half_y, q_send, q_recv, sib)
    done.wait()


def solution(mesh):
    def step(x, w_gate, w_up, w_down):
        rows, depth = x.shape
        hidden = w_gate.shape[1]
        n_chunks, n_gu, n_dn = rows // M, hidden // TH, depth // W
        dma = pltpu.SemaphoreType.DMA
        y = pl.pallas_call(
            functools.partial(kernel, n_chunks, n_gu, n_dn),
            out_shape=jax.ShapeDtypeStruct((rows, depth), BF16),
            in_specs=[pl.BlockSpec(memory_space=pl.ANY)] * 4,
            out_specs=pl.BlockSpec(memory_space=pl.ANY),
            scratch_shapes=[
                pltpu.VMEM((M, depth), BF16),
                pltpu.VMEM((2, depth, 2 * TH), BF16),
                pltpu.VMEM((M, 2 * TH), F32),
                pltpu.VMEM((M, hidden), BF16),
                pltpu.VMEM((n_dn, hidden, W), BF16),
                pltpu.VMEM((n_dn, HALF, W), F32),
                pltpu.VMEM((n_dn, HALF, W), BF16),
                pltpu.VMEM((n_dn, HALF, W), BF16),
                pltpu.VMEM((4, QUARTER, W), F32),
                pltpu.VMEM((4, QUARTER, W), BF16),
                pltpu.VMEM((4, QUARTER, W), BF16),
                pltpu.VMEM((4, EIGHTH, W), F32),
                pltpu.VMEM((4, EIGHTH, W), BF16),
                pltpu.VMEM((4, EIGHTH, W), BF16),
                pltpu.VMEM((4, EIGHTH, W), BF16),
                dma((2,)), dma((2, 2, 2)), dma((n_dn,)),
                dma((n_dn,)), dma((n_dn,)),
                dma((4,)), dma((4,)),
                dma((4,)), dma((4,)),
                dma((4,)),
                dma((4,)), dma((4,)),
                dma((4,)), dma((8,)),
                dma((4,)), dma((8,)),
                dma, dma,
                pltpu.SemaphoreType.REGULAR,
            ],
            compiler_params=pltpu.CompilerParams(
                collective_id=0, has_side_effects=True, vmem_limit_bytes=67043328
            ),
        )(x, w_gate, w_up, w_down)
        return y

    return jax.shard_map(
        step,
        mesh=mesh,
        in_specs=(P("dp", None), P(None, "tp"), P(None, "tp"), P("tp", None)),
        out_specs=P("dp", None),
        check_vma=False,
    )
```

```python
import functools

import jax
import jax.numpy as jnp
from jax import lax
from jax.experimental import pallas as pl
from jax.experimental.pallas import tpu as pltpu
from jax.sharding import PartitionSpec as P

MESH = pl.DeviceIdType.MESH
BF16, F32 = jnp.bfloat16, jnp.float32
M = 256
HALF, QUARTER, EIGHTH = M // 2, M // 4, M // 8
TH = 256
W = 1024
RK = 3
L2, L3, L4, L5 = 2, 4, 6, 8


def kernel(
    n_chunks, n_gu, n_dn,
    x_hbm, wg_hbm, wu_hbm, wd_hbm, y_hbm,
    xbuf, wbuf, acc, hbuf, wdbuf, keep, sp, rp, k1, s1, r1, k2, s2, r2, fin,
    x_sem, w_sem, wd_sem, p_send, p_recv, a_send, a_recv, b_send, b_recv,
    g_send, g1_recv, g_recv, q_send, q_recv,
):
    me = lax.axis_index("tp")
    dx, dy, dc = me // 4, (me // 2) % 2, me % 2
    sib = me + 1 - 2 * dc
    kh = x_hbm.shape[1] // 2
    n_tiles = n_chunks * n_gu
    n_units = n_chunks * n_dn

    def remote(src, dst, send, recv, dev):
        return pltpu.make_async_remote_copy(
            src_ref=src, dst_ref=dst, send_sem=send, recv_sem=recv, device_id={"tp": dev}, device_id_type=MESH
        )

    def w_copies(t, part):
        col = pl.multiple_of((t % n_gu) * TH, TH)
        rows = pl.ds(part * kh, kh)
        slot = t % 2
        return [
            pltpu.make_async_copy(
                src.at[rows, pl.ds(col, TH)], wbuf.at[slot, rows, pl.ds(TH * n, TH)], w_sem.at[slot, part, n]
            )
            for n, src in enumerate((wg_hbm, wu_hbm))
        ]

    def x_copies(k):
        own = pl.multiple_of(k * M + dc * HALF, HALF)
        other = pl.multiple_of(k * M + (1 - dc) * HALF, HALF)
        s = k % 2
        return [
            pltpu.make_async_copy(x_hbm.at[pl.ds(own, HALF)], xbuf.at[s, pl.ds(0, HALF)], x_sem.at[s, 0]),
            pltpu.make_async_copy(x_hbm.at[pl.ds(other, HALF)], xbuf.at[s, pl.ds(HALF, HALF)], x_sem.at[s, 1]),
        ]

    def wd_copy(j):
        return pltpu.make_async_copy(
            wd_hbm.at[:, pl.ds(pl.multiple_of(j * W, W), W)], wdbuf.at[j], wd_sem.at[j]
        )

    def pair_copy(u):
        j = u % RK
        return remote(sp.at[j], rp.at[j], p_send.at[j], p_recv.at[j], sib)

    def place(u):
        e = u % 2
        xa, ya = dx + (1 - e) * (1 - 2 * dx), dy + e * (1 - 2 * dy)
        xb, yb = dx + e * (1 - 2 * dx), dy + (1 - e) * (1 - 2 * dy)
        p, r = dx * (1 - e) + dy * e, dx * e + dy * (1 - e)
        return 4 * xa + 2 * ya + dc, 4 * xb + 2 * yb + dc, p, r

    def block(u, p, r):
        row = pl.multiple_of((u // n_dn) * M + dc * HALF + p * QUARTER + r * EIGHTH, EIGHTH)
        return y_hbm.at[pl.ds(row, EIGHTH), pl.ds(pl.multiple_of((u % n_dn) * W, W), W)]

    def half_block(u):
        row = pl.multiple_of((u // n_dn) * M + dc * HALF, HALF)
        return y_hbm.at[pl.ds(row, HALF), pl.ds(pl.multiple_of((u % n_dn) * W, W), W)]

    def a_copy(u):
        a, _, _, _ = place(u)
        s = u % 4
        return remote(s1.at[s], r1.at[s], a_send.at[s], a_recv.at[s], a)

    def b_copy(u):
        _, b, _, _ = place(u)
        s = u % 4
        return remote(s2.at[s], r2.at[s], b_send.at[s], b_recv.at[s], b)

    def loc_copy(u):
        _, _, p, r = place(u)
        return pltpu.make_async_copy(fin.at[u % 4], block(u, p, r), g_send.at[u % 4])

    def g1_copy(u):
        _, b, p, r = place(u)
        return remote(fin.at[u % 4], block(u, p, r), g_send.at[u % 4], g1_recv.at[u % 8], b)

    def g2_copy(u):
        a, _, p, r = place(u)
        return remote(fin.at[u % 4], block(u, p, r), g_send.at[u % 4], g_recv.at[u % 8], a)

    def g3_copy(u):
        a, _, p, r = place(u)
        blk = block(u, p, 1 - r)
        return remote(blk, blk, g_send.at[u % 4], g_recv.at[u % 8], a)

    def q_copy(u):
        blk = half_block(u)
        return remote(blk, blk, q_send, q_recv, sib)

    def step1(u):
        pair_copy(u).wait()
        s, j = u % 4, u % RK
        _, _, p, _ = place(u)
        mine = pl.ds(pl.multiple_of(p * QUARTER, QUARTER), QUARTER)
        theirs = pl.ds(pl.multiple_of((1 - p) * QUARTER, QUARTER), QUARTER)
        s1[s] = (keep[j, theirs] + rp[j, theirs].astype(F32)).astype(BF16)
        k1[s] = keep[j, mine] + rp[j, mine].astype(F32)

    def step2(u):
        a_copy(u).wait()
        s = u % 4
        _, _, _, r = place(u)
        mine = pl.ds(pl.multiple_of(r * EIGHTH, EIGHTH), EIGHTH)
        theirs = pl.ds(pl.multiple_of((1 - r) * EIGHTH, EIGHTH), EIGHTH)
        s2[s] = (k1[s, theirs] + r1[s, theirs].astype(F32)).astype(BF16)
        k2[s] = k1[s, mine] + r1[s, mine].astype(F32)

    def step3(u):
        b_copy(u).wait()
        s = u % 4
        fin[s] = (k2[s] + r2[s].astype(F32)).astype(BF16)

    def step4(u):
        g1_copy(u).wait_recv()

    def step5(u):
        a, _, p, _ = place(u)
        whole = half_block(u)
        remote(whole, whole, g_send.at[u % 4], g_recv.at[u % 8], a).wait_send()
        row = pl.multiple_of((u // n_dn) * M + dc * HALF + (1 - p) * QUARTER, QUARTER)
        two = y_hbm.at[pl.ds(row, QUARTER), pl.ds(pl.multiple_of((u % n_dn) * W, W), W)]
        remote(two, two, g_send.at[u % 4], g_recv.at[u % 8], a).wait_recv()

    def tick(n):
        u5, u4, u3, u2, u1 = n - L5, n - L4, n - L3, n - L2, n
        steady = (u5 >= 0) & (u1 < n_units)

        @pl.when(steady)
        def _():
            step5(u5)
            step4(u4)
            step3(u3)
            step2(u2)
            step1(u1)
            a_copy(u1).start()
            b_copy(u2).start()
            g1_copy(u3).start()
            g3_copy(u4).start()
            g2_copy(u3).start()
            loc_copy(u3).start()
            q_copy(u5).start()

        @pl.when(jnp.logical_not(steady))
        def _():
            @pl.when((u5 >= 0) & (u5 < n_units))
            def _():
                step5(u5)
                q_copy(u5).start()

            @pl.when((u4 >= 0) & (u4 < n_units))
            def _():
                step4(u4)
                g3_copy(u4).start()

            @pl.when((u3 >= 0) & (u3 < n_units))
            def _():
                step3(u3)
                g1_copy(u3).start()
                g2_copy(u3).start()
                loc_copy(u3).start()

            @pl.when((u2 >= 0) & (u2 < n_units))
            def _():
                step2(u2)
                b_copy(u2).start()

            @pl.when((u1 >= 0) & (u1 < n_units))
            def _():
                step1(u1)
                a_copy(u1).start()

    def start(copies):
        for c in copies:
            c.start()

    def wait(copies):
        for c in copies:
            c.wait()

    def hidden_step(k, i):
        t = k * n_gu + i
        slot, xs = t % 2, k % 2

        def refill(part):
            @pl.when(t + 2 < n_tiles)
            def _():
                start(w_copies(t + 2, part))

        wait(w_copies(t, 0))
        acc[...] = jnp.dot(xbuf[xs, :, :kh], wbuf[slot, :kh], preferred_element_type=F32)
        refill(0)
        wait(w_copies(t, 1))
        gu = acc[...] + jnp.dot(xbuf[xs, :, kh:], wbuf[slot, kh:], preferred_element_type=F32)
        g, up = gu[:, :TH], gu[:, TH:]
        hbuf[xs, :, pl.ds(pl.multiple_of(i * TH, TH), TH)] = (g * jax.nn.sigmoid(g) * up).astype(BF16)
        refill(1)

    def term_step(k, j):
        u = k * n_dn + j
        tick(u - 1)

        @pl.when(k == 0)
        def _():
            wd_copy(j).wait()

            @pl.when(j + 2 < n_dn)
            def _():
                wd_copy(j + 2).start()

        term = jnp.dot(hbuf[k % 2], wdbuf[j], preferred_element_type=F32)
        sp[u % RK] = term[HALF:].astype(BF16)
        keep[u % RK] = term[:HALF]
        pair_copy(u).start()

    start(x_copies(0))
    for t in range(2):
        for part in range(2):
            start(w_copies(t, part))

    barrier = pltpu.get_barrier_semaphore()
    partners = (sib, 4 * (1 - dx) + 2 * dy + dc, 4 * dx + 2 * (1 - dy) + dc)
    for dev in partners:
        pl.semaphore_signal(barrier, inc=1, device_id={"tp": dev}, device_id_type=MESH)
    pl.semaphore_wait(barrier, 3)

    def chunk(k, _):
        wait(x_copies(k))

        @pl.when((k > 0) & (k + 1 < n_chunks))
        def _():
            start(x_copies(k + 1))

        def both(i, _):
            @pl.when((k > 0) & (i % 4 != 3))
            def _():
                term_step(k - 1, i - i // 4)

            hidden_step(k, i)
            return 0

        lax.fori_loop(0, n_gu, both, 0)

        @pl.when(k == 0)
        def _():
            start([wd_copy(0), wd_copy(1)])
            start(x_copies(1))

        return 0

    lax.fori_loop(0, n_chunks, chunk, 0)

    def term_only(j, _):
        term_step(n_chunks - 1, j)
        return 0

    lax.fori_loop(0, n_dn, term_only, 0)

    def last(n, _):
        tick(n)
        return 0

    lax.fori_loop(n_units - 1, n_units + L5, last, 0)
    half_y = y_hbm.at[pl.ds(0, y_hbm.shape[0] // 2)]
    remote(half_y, half_y, q_send, q_recv, sib).wait()


def solution(mesh):
    def step(x, w_gate, w_up, w_down):
        rows, depth = x.shape
        hidden = w_gate.shape[1]
        n_chunks, n_gu, n_dn = rows // M, hidden // TH, depth // W
        dma = pltpu.SemaphoreType.DMA
        y = pl.pallas_call(
            functools.partial(kernel, n_chunks, n_gu, n_dn),
            out_shape=jax.ShapeDtypeStruct((rows, depth), BF16),
            in_specs=[pl.BlockSpec(memory_space=pl.ANY)] * 4,
            out_specs=pl.BlockSpec(memory_space=pl.ANY),
            scratch_shapes=[
                pltpu.VMEM((2, M, depth), BF16),
                pltpu.VMEM((2, depth, 2 * TH), BF16),
                pltpu.VMEM((M, 2 * TH), F32),
                pltpu.VMEM((2, M, hidden), BF16),
                pltpu.VMEM((n_dn, hidden, W), BF16),
                pltpu.VMEM((RK, HALF, W), F32),
                pltpu.VMEM((RK, HALF, W), BF16),
                pltpu.VMEM((RK, HALF, W), BF16),
                pltpu.VMEM((4, QUARTER, W), F32),
                pltpu.VMEM((4, QUARTER, W), BF16),
                pltpu.VMEM((4, QUARTER, W), BF16),
                pltpu.VMEM((4, EIGHTH, W), F32),
                pltpu.VMEM((4, EIGHTH, W), BF16),
                pltpu.VMEM((4, EIGHTH, W), BF16),
                pltpu.VMEM((4, EIGHTH, W), BF16),
                dma((2, 2)), dma((2, 2, 2)), dma((n_dn,)),
                dma((RK,)), dma((RK,)),
                dma((4,)), dma((4,)),
                dma((4,)), dma((4,)),
                dma((4,)), dma((8,)), dma((8,)),
                dma, dma,
            ],
            compiler_params=pltpu.CompilerParams(
                collective_id=0, has_side_effects=True, vmem_limit_bytes=67043328
            ),
        )(x, w_gate, w_up, w_down)
        return y

    return jax.shard_map(
        step,
        mesh=mesh,
        in_specs=(P("dp", None), P(None, "tp"), P(None, "tp"), P("tp", None)),
        out_specs=P("dp", None),
        check_vma=False,
    )
```

```python
import functools

import jax
import jax.numpy as jnp
from jax import lax
from jax.experimental import pallas as pl
from jax.experimental.pallas import tpu as pltpu
from jax.sharding import PartitionSpec as P

MESH = pl.DeviceIdType.MESH
BF16, F32 = jnp.bfloat16, jnp.float32
M = 256
HALF, QUARTER, EIGHTH = M // 2, M // 4, M // 8
TH = 256
W = 1024
RK = 4
L2, L3, L4, L5 = 2, 4, 6, 8


def kernel(
    n_chunks, n_gu, n_dn,
    x_hbm, wg_hbm, wu_hbm, wd_hbm, y_hbm,
    xbuf, wbuf, acc, hbuf, wdbuf, keep, sp, rp, k1, s1, r1, k2, s2, r2, fin,
    x_sem, w_sem, wd_sem, p_send, p_recv, a_send, a_recv, b_send, b_recv,
    g_send, g1_recv, g_recv, q_send, q_recv,
):
    me = lax.axis_index("tp")
    dx, dy, dc = me // 4, (me // 2) % 2, me % 2
    sib = me + 1 - 2 * dc
    kh = x_hbm.shape[1] // 2
    n_tiles = n_chunks * n_gu
    n_units = n_chunks * n_dn

    def chunk_of(u):
        return lax.div(u * (65536 // n_dn + 1), 65536)

    def column_of(u):
        return u - chunk_of(u) * n_dn

    def remote(src, dst, send, recv, dev):
        return pltpu.make_async_remote_copy(
            src_ref=src, dst_ref=dst, send_sem=send, recv_sem=recv, device_id={"tp": dev}, device_id_type=MESH
        )

    def w_copies(t, part):
        col = pl.multiple_of((t % n_gu) * TH, TH)
        rows = pl.ds(part * kh, kh)
        slot = t % 2
        return [
            pltpu.make_async_copy(
                src.at[rows, pl.ds(col, TH)], wbuf.at[slot, rows, pl.ds(TH * n, TH)], w_sem.at[slot, part, n]
            )
            for n, src in enumerate((wg_hbm, wu_hbm))
        ]

    def x_copies(k):
        own = pl.multiple_of(k * M + dc * HALF, HALF)
        other = pl.multiple_of(k * M + (1 - dc) * HALF, HALF)
        s = k % 2
        return [
            pltpu.make_async_copy(x_hbm.at[pl.ds(own, HALF)], xbuf.at[s, pl.ds(0, HALF)], x_sem.at[s, 0]),
            pltpu.make_async_copy(x_hbm.at[pl.ds(other, HALF)], xbuf.at[s, pl.ds(HALF, HALF)], x_sem.at[s, 1]),
        ]

    def wd_copy(j):
        return pltpu.make_async_copy(
            wd_hbm.at[:, pl.ds(pl.multiple_of(j * W, W), W)], wdbuf.at[j], wd_sem.at[j]
        )

    def pair_copy(u):
        j = lax.rem(u, RK)
        return remote(sp.at[j], rp.at[j], p_send.at[j], p_recv.at[j], sib)

    def place(u):
        e = lax.rem(u, 2)
        xa, ya = dx + (1 - e) * (1 - 2 * dx), dy + e * (1 - 2 * dy)
        xb, yb = dx + e * (1 - 2 * dx), dy + (1 - e) * (1 - 2 * dy)
        p, r = dx * (1 - e) + dy * e, dx * e + dy * (1 - e)
        return 4 * xa + 2 * ya + dc, 4 * xb + 2 * yb + dc, p, r

    def block(u, p, r):
        row = pl.multiple_of(chunk_of(u) * M + dc * HALF + p * QUARTER + r * EIGHTH, EIGHTH)
        return y_hbm.at[pl.ds(row, EIGHTH), pl.ds(pl.multiple_of(column_of(u) * W, W), W)]

    def half_block(u):
        row = pl.multiple_of(chunk_of(u) * M + dc * HALF, HALF)
        return y_hbm.at[pl.ds(row, HALF), pl.ds(pl.multiple_of(column_of(u) * W, W), W)]

    def a_copy(u):
        a, _, _, _ = place(u)
        s = lax.rem(u, 4)
        return remote(s1.at[s], r1.at[s], a_send.at[s], a_recv.at[s], a)

    def b_copy(u):
        _, b, _, _ = place(u)
        s = lax.rem(u, 4)
        return remote(s2.at[s], r2.at[s], b_send.at[s], b_recv.at[s], b)

    def loc_copy(u):
        _, _, p, r = place(u)
        return pltpu.make_async_copy(fin.at[lax.rem(u, 4)], block(u, p, r), g_send.at[lax.rem(u, 4)])

    def g1_copy(u):
        _, b, p, r = place(u)
        return remote(fin.at[lax.rem(u, 4)], block(u, p, r), g_send.at[lax.rem(u, 4)], g1_recv.at[lax.rem(u, 8)], b)

    def g2_copy(u):
        a, _, p, r = place(u)
        return remote(fin.at[lax.rem(u, 4)], block(u, p, r), g_send.at[lax.rem(u, 4)], g_recv.at[lax.rem(u, 8)], a)

    def g3_copy(u):
        a, _, p, r = place(u)
        blk = block(u, p, 1 - r)
        return remote(blk, blk, g_send.at[lax.rem(u, 4)], g_recv.at[lax.rem(u, 8)], a)

    def q_copy(u):
        blk = half_block(u)
        return remote(blk, blk, q_send, q_recv, sib)

    def step1(u):
        pair_copy(u).wait()
        s, j = lax.rem(u, 4), lax.rem(u, RK)
        _, _, p, _ = place(u)
        mine = pl.ds(pl.multiple_of(p * QUARTER, QUARTER), QUARTER)
        theirs = pl.ds(pl.multiple_of((1 - p) * QUARTER, QUARTER), QUARTER)
        s1[s] = (keep[j, theirs] + rp[j, theirs].astype(F32)).astype(BF16)
        k1[s] = keep[j, mine] + rp[j, mine].astype(F32)

    def step2(u):
        a_copy(u).wait()
        s = lax.rem(u, 4)
        _, _, _, r = place(u)
        mine = pl.ds(pl.multiple_of(r * EIGHTH, EIGHTH), EIGHTH)
        theirs = pl.ds(pl.multiple_of((1 - r) * EIGHTH, EIGHTH), EIGHTH)
        s2[s] = (k1[s, theirs] + r1[s, theirs].astype(F32)).astype(BF16)
        k2[s] = k1[s, mine] + r1[s, mine].astype(F32)

    def step3(u):
        b_copy(u).wait()
        s = lax.rem(u, 4)
        fin[s] = (k2[s] + r2[s].astype(F32)).astype(BF16)

    def step4(u):
        g1_copy(u).wait_recv()

    def step5(u):
        a, _, p, _ = place(u)
        whole = half_block(u)
        remote(whole, whole, g_send.at[lax.rem(u, 4)], g_recv.at[lax.rem(u, 8)], a).wait_send()
        row = pl.multiple_of(chunk_of(u) * M + dc * HALF + (1 - p) * QUARTER, QUARTER)
        two = y_hbm.at[pl.ds(row, QUARTER), pl.ds(pl.multiple_of(column_of(u) * W, W), W)]
        remote(two, two, g_send.at[lax.rem(u, 4)], g_recv.at[lax.rem(u, 8)], a).wait_recv()

    def tick(n):
        u5, u4, u3, u2, u1 = n - L5, n - L4, n - L3, n - L2, n
        steady = (u5 >= 0) & (u1 < n_units)

        @pl.when(steady)
        def _():
            step5(u5)
            step4(u4)
            step3(u3)
            step2(u2)
            step1(u1)
            a_copy(u1).start()
            b_copy(u2).start()
            g1_copy(u3).start()
            g3_copy(u4).start()
            g2_copy(u3).start()
            loc_copy(u3).start()
            q_copy(u5).start()

        @pl.when(jnp.logical_not(steady))
        def _():
            @pl.when((u5 >= 0) & (u5 < n_units))
            def _():
                step5(u5)
                q_copy(u5).start()

            @pl.when((u4 >= 0) & (u4 < n_units))
            def _():
                step4(u4)
                g3_copy(u4).start()

            @pl.when((u3 >= 0) & (u3 < n_units))
            def _():
                step3(u3)
                g1_copy(u3).start()
                g2_copy(u3).start()
                loc_copy(u3).start()

            @pl.when((u2 >= 0) & (u2 < n_units))
            def _():
                step2(u2)
                b_copy(u2).start()

            @pl.when((u1 >= 0) & (u1 < n_units))
            def _():
                step1(u1)
                a_copy(u1).start()

    def start(copies):
        for c in copies:
            c.start()

    def wait(copies):
        for c in copies:
            c.wait()

    def hidden_step(k, i):
        t = k * n_gu + i
        slot, xs = t % 2, k % 2

        def refill(part):
            @pl.when(t + 2 < n_tiles)
            def _():
                start(w_copies(t + 2, part))

        wait(w_copies(t, 0))
        acc[...] = jnp.dot(xbuf[xs, :, :kh], wbuf[slot, :kh], preferred_element_type=F32)
        refill(0)
        wait(w_copies(t, 1))
        gu = acc[...] + jnp.dot(xbuf[xs, :, kh:], wbuf[slot, kh:], preferred_element_type=F32)
        g, up = gu[:, :TH], gu[:, TH:]
        hbuf[xs, :, pl.ds(pl.multiple_of(i * TH, TH), TH)] = (g * jax.nn.sigmoid(g) * up).astype(BF16)
        refill(1)

    def term_step(k, j):
        u = k * n_dn + j
        tick(u - 1)

        @pl.when(k == 0)
        def _():
            wd_copy(j).wait()

            @pl.when(j + 2 < n_dn)
            def _():
                wd_copy(j + 2).start()

        term = jnp.dot(hbuf[k % 2], wdbuf[j], preferred_element_type=F32)
        sp[lax.rem(u, RK)] = term[HALF:].astype(BF16)
        keep[lax.rem(u, RK)] = term[:HALF]
        pair_copy(u).start()

    start(x_copies(0))
    for t in range(2):
        for part in range(2):
            start(w_copies(t, part))

    barrier = pltpu.get_barrier_semaphore()
    partners = (sib, 4 * (1 - dx) + 2 * dy + dc, 4 * dx + 2 * (1 - dy) + dc)
    for dev in partners:
        pl.semaphore_signal(barrier, inc=1, device_id={"tp": dev}, device_id_type=MESH)
    pl.semaphore_wait(barrier, 3)

    def chunk(k, _):
        wait(x_copies(k))

        @pl.when((k > 0) & (k + 1 < n_chunks))
        def _():
            start(x_copies(k + 1))

        def both(i, _):
            @pl.when((k > 0) & (i % 4 != 3))
            def _():
                term_step(k - 1, i - i // 4)

            @pl.when((k == 0) & (i == n_gu - 3))
            def _():
                start(x_copies(1))
                wd_copy(0).start()

            @pl.when((k == 0) & (i == n_gu - 1))
            def _():
                wd_copy(1).start()

            hidden_step(k, i)
            return 0

        lax.fori_loop(0, n_gu, both, 0)

        return 0

    lax.fori_loop(0, n_chunks, chunk, 0)

    def term_only(j, _):
        term_step(n_chunks - 1, j)
        return 0

    lax.fori_loop(0, n_dn, term_only, 0)

    def last(n, _):
        tick(n)
        return 0

    lax.fori_loop(n_units - 1, n_units + L5, last, 0)
    half_y = y_hbm.at[pl.ds(0, y_hbm.shape[0] // 2)]
    remote(half_y, half_y, q_send, q_recv, sib).wait()


def solution(mesh):
    def step(x, w_gate, w_up, w_down):
        rows, depth = x.shape
        hidden = w_gate.shape[1]
        n_chunks, n_gu, n_dn = rows // M, hidden // TH, depth // W
        dma = pltpu.SemaphoreType.DMA
        y = pl.pallas_call(
            functools.partial(kernel, n_chunks, n_gu, n_dn),
            out_shape=jax.ShapeDtypeStruct((rows, depth), BF16),
            in_specs=[pl.BlockSpec(memory_space=pl.ANY)] * 4,
            out_specs=pl.BlockSpec(memory_space=pl.ANY),
            scratch_shapes=[
                pltpu.VMEM((2, M, depth), BF16),
                pltpu.VMEM((2, depth, 2 * TH), BF16),
                pltpu.VMEM((M, 2 * TH), F32),
                pltpu.VMEM((2, M, hidden), BF16),
                pltpu.VMEM((n_dn, hidden, W), BF16),
                pltpu.VMEM((RK, HALF, W), F32),
                pltpu.VMEM((RK, HALF, W), BF16),
                pltpu.VMEM((RK, HALF, W), BF16),
                pltpu.VMEM((4, QUARTER, W), F32),
                pltpu.VMEM((4, QUARTER, W), BF16),
                pltpu.VMEM((4, QUARTER, W), BF16),
                pltpu.VMEM((4, EIGHTH, W), F32),
                pltpu.VMEM((4, EIGHTH, W), BF16),
                pltpu.VMEM((4, EIGHTH, W), BF16),
                pltpu.VMEM((4, EIGHTH, W), BF16),
                dma((2, 2)), dma((2, 2, 2)), dma((n_dn,)),
                dma((RK,)), dma((RK,)),
                dma((4,)), dma((4,)),
                dma((4,)), dma((4,)),
                dma((4,)), dma((8,)), dma((8,)),
                dma, dma,
            ],
            compiler_params=pltpu.CompilerParams(
                collective_id=0, has_side_effects=True, vmem_limit_bytes=67043328
            ),
        )(x, w_gate, w_up, w_down)
        return y

    return jax.shard_map(
        step,
        mesh=mesh,
        in_specs=(P("dp", None), P(None, "tp"), P(None, "tp"), P("tp", None)),
        out_specs=P("dp", None),
        check_vma=False,
    )
```

```python
import functools

import jax
import jax.numpy as jnp
from jax import lax
from jax.experimental import pallas as pl
from jax.experimental.pallas import tpu as pltpu
from jax.sharding import PartitionSpec as P

MESH = pl.DeviceIdType.MESH
BF16, F32 = jnp.bfloat16, jnp.float32
M = 256
HALF, QUARTER, EIGHTH = M // 2, M // 4, M // 8
TH = 256
W = 1024
RK = 4
L2, L3, L4, L5 = 2, 4, 6, 8


def kernel(
    n_chunks, n_gu, n_dn,
    x_hbm, wg_hbm, wu_hbm, wd_hbm, y_hbm,
    xbuf, wbuf, acc, hbuf, wdbuf, keep, sp, rp, k1, s1, r1, k2, s2, r2, fin,
    x_sem, w_sem, wd_sem, p_send, p_recv, a_send, a_recv, b_send, b_recv,
    g_send, g1_recv, g_recv, q_send, q_recv,
):
    me = lax.axis_index("tp")
    dx, dy, dc = me // 4, (me // 2) % 2, me % 2
    sib = me + 1 - 2 * dc
    kh = x_hbm.shape[1] // 2
    n_tiles = n_chunks * n_gu
    n_units = n_chunks * n_dn

    def chunk_of(u):
        return lax.div(u * (65536 // n_dn + 1), 65536)

    def column_of(u):
        return u - chunk_of(u) * n_dn

    def remote(src, dst, send, recv, dev):
        return pltpu.make_async_remote_copy(
            src_ref=src, dst_ref=dst, send_sem=send, recv_sem=recv, device_id={"tp": dev}, device_id_type=MESH
        )

    def w_copies(t, part):
        col = pl.multiple_of((t % n_gu) * TH, TH)
        rows = pl.ds(part * kh, kh)
        slot = t % 2
        return [
            pltpu.make_async_copy(
                src.at[rows, pl.ds(col, TH)], wbuf.at[slot, rows, pl.ds(TH * n, TH)], w_sem.at[slot, part, n]
            )
            for n, src in enumerate((wg_hbm, wu_hbm))
        ]

    def x_copies(k):
        own = pl.multiple_of(k * M + dc * HALF, HALF)
        other = pl.multiple_of(k * M + (1 - dc) * HALF, HALF)
        s = k % 2
        return [
            pltpu.make_async_copy(x_hbm.at[pl.ds(own, HALF)], xbuf.at[s, pl.ds(0, HALF)], x_sem.at[s, 0]),
            pltpu.make_async_copy(x_hbm.at[pl.ds(other, HALF)], xbuf.at[s, pl.ds(HALF, HALF)], x_sem.at[s, 1]),
        ]

    def wd_copy(j):
        return pltpu.make_async_copy(
            wd_hbm.at[:, pl.ds(pl.multiple_of(j * W, W), W)], wdbuf.at[j], wd_sem.at[j]
        )

    def pair_copy(u):
        j = lax.rem(u, RK)
        return remote(sp.at[j], rp.at[j], p_send.at[j], p_recv.at[j], sib)

    def place(u):
        e = lax.rem(u, 2)
        xa, ya = dx + (1 - e) * (1 - 2 * dx), dy + e * (1 - 2 * dy)
        xb, yb = dx + e * (1 - 2 * dx), dy + (1 - e) * (1 - 2 * dy)
        p, r = dx * (1 - e) + dy * e, dx * e + dy * (1 - e)
        return 4 * xa + 2 * ya + dc, 4 * xb + 2 * yb + dc, p, r

    def block(u, p, r):
        row = pl.multiple_of(chunk_of(u) * M + dc * HALF + p * QUARTER + r * EIGHTH, EIGHTH)
        return y_hbm.at[pl.ds(row, EIGHTH), pl.ds(pl.multiple_of(column_of(u) * W, W), W)]

    def half_block(u):
        row = pl.multiple_of(chunk_of(u) * M + dc * HALF, HALF)
        return y_hbm.at[pl.ds(row, HALF), pl.ds(pl.multiple_of(column_of(u) * W, W), W)]

    def a_copy(u):
        a, _, _, _ = place(u)
        s = lax.rem(u, 4)
        return remote(s1.at[s], r1.at[s], a_send.at[s], a_recv.at[s], a)

    def b_copy(u):
        _, b, _, _ = place(u)
        s = lax.rem(u, 4)
        return remote(s2.at[s], r2.at[s], b_send.at[s], b_recv.at[s], b)

    def loc_copy(u):
        _, _, p, r = place(u)
        return pltpu.make_async_copy(fin.at[lax.rem(u, 4)], block(u, p, r), g_send.at[lax.rem(u, 4)])

    def g1_copy(u):
        _, b, p, r = place(u)
        return remote(fin.at[lax.rem(u, 4)], block(u, p, r), g_send.at[lax.rem(u, 4)], g1_recv.at[lax.rem(u, 8)], b)

    def g2_copy(u):
        a, _, p, r = place(u)
        return remote(fin.at[lax.rem(u, 4)], block(u, p, r), g_send.at[lax.rem(u, 4)], g_recv.at[lax.rem(u, 8)], a)

    def g3_copy(u):
        a, _, p, r = place(u)
        blk = block(u, p, 1 - r)
        return remote(blk, blk, g_send.at[lax.rem(u, 4)], g_recv.at[lax.rem(u, 8)], a)

    def q_copy(u):
        blk = half_block(u)
        return remote(blk, blk, q_send, q_recv, sib)

    def step1(u):
        pair_copy(u).wait()
        s, j = lax.rem(u, 4), lax.rem(u, RK)
        _, _, p, _ = place(u)
        mine = pl.ds(pl.multiple_of(p * QUARTER, QUARTER), QUARTER)
        theirs = pl.ds(pl.multiple_of((1 - p) * QUARTER, QUARTER), QUARTER)
        s1[s] = (keep[j, theirs] + rp[j, theirs].astype(F32)).astype(BF16)
        k1[s] = keep[j, mine] + rp[j, mine].astype(F32)

    def step2(u):
        a_copy(u).wait()
        s = lax.rem(u, 4)
        _, _, _, r = place(u)
        mine = pl.ds(pl.multiple_of(r * EIGHTH, EIGHTH), EIGHTH)
        theirs = pl.ds(pl.multiple_of((1 - r) * EIGHTH, EIGHTH), EIGHTH)
        s2[s] = (k1[s, theirs] + r1[s, theirs].astype(F32)).astype(BF16)
        k2[s] = k1[s, mine] + r1[s, mine].astype(F32)

    def step3(u):
        b_copy(u).wait()
        s = lax.rem(u, 4)
        fin[s] = (k2[s] + r2[s].astype(F32)).astype(BF16)

    def step4(u):
        g1_copy(u).wait_recv()

    def step5(u):
        a, _, p, _ = place(u)
        whole = half_block(u)
        remote(whole, whole, g_send.at[lax.rem(u, 4)], g_recv.at[lax.rem(u, 8)], a).wait_send()
        row = pl.multiple_of(chunk_of(u) * M + dc * HALF + (1 - p) * QUARTER, QUARTER)
        two = y_hbm.at[pl.ds(row, QUARTER), pl.ds(pl.multiple_of(column_of(u) * W, W), W)]
        remote(two, two, g_send.at[lax.rem(u, 4)], g_recv.at[lax.rem(u, 8)], a).wait_recv()

    def tick(n):
        u5, u4, u3, u2, u1 = n - L5, n - L4, n - L3, n - L2, n
        steady = (u5 >= 0) & (u1 < n_units)

        @pl.when(steady)
        def _():
            step5(u5)
            step1(u1)
            step2(u2)
            step3(u3)
            step4(u4)
            a_copy(u1).start()
            b_copy(u2).start()
            g1_copy(u3).start()
            g3_copy(u4).start()
            g2_copy(u3).start()
            loc_copy(u3).start()
            q_copy(u5).start()

        @pl.when(jnp.logical_not(steady))
        def _():
            @pl.when((u5 >= 0) & (u5 < n_units))
            def _():
                step5(u5)
                q_copy(u5).start()

            @pl.when((u4 >= 0) & (u4 < n_units))
            def _():
                step4(u4)
                g3_copy(u4).start()

            @pl.when((u3 >= 0) & (u3 < n_units))
            def _():
                step3(u3)
                g1_copy(u3).start()
                g2_copy(u3).start()
                loc_copy(u3).start()

            @pl.when((u2 >= 0) & (u2 < n_units))
            def _():
                step2(u2)
                b_copy(u2).start()

            @pl.when((u1 >= 0) & (u1 < n_units))
            def _():
                step1(u1)
                a_copy(u1).start()

    def start(copies):
        for c in copies:
            c.start()

    def wait(copies):
        for c in copies:
            c.wait()

    def hidden_step(k, i):
        t = k * n_gu + i
        slot, xs = t % 2, k % 2

        def refill(part):
            @pl.when(t + 2 < n_tiles)
            def _():
                start(w_copies(t + 2, part))

        wait(w_copies(t, 0))
        acc[...] = jnp.dot(xbuf[xs, :, :kh], wbuf[slot, :kh], preferred_element_type=F32)
        refill(0)
        wait(w_copies(t, 1))
        gu = acc[...] + jnp.dot(xbuf[xs, :, kh:], wbuf[slot, kh:], preferred_element_type=F32)
        g, up = gu[:, :TH], gu[:, TH:]
        hbuf[xs, :, pl.ds(pl.multiple_of(i * TH, TH), TH)] = (g * jax.nn.sigmoid(g) * up).astype(BF16)
        refill(1)

    def term_step(k, j):
        u = k * n_dn + j
        tick(u - 1)

        @pl.when(k == 0)
        def _():
            wd_copy(j).wait()

            @pl.when(j + 2 < n_dn)
            def _():
                wd_copy(j + 2).start()

        term = jnp.dot(hbuf[k % 2], wdbuf[j], preferred_element_type=F32)
        sp[lax.rem(u, RK)] = term[HALF:].astype(BF16)
        keep[lax.rem(u, RK)] = term[:HALF]
        pair_copy(u).start()

    start(x_copies(0))
    for t in range(2):
        for part in range(2):
            start(w_copies(t, part))

    barrier = pltpu.get_barrier_semaphore()
    partners = (sib, 4 * (1 - dx) + 2 * dy + dc, 4 * dx + 2 * (1 - dy) + dc)
    for dev in partners:
        pl.semaphore_signal(barrier, inc=1, device_id={"tp": dev}, device_id_type=MESH)
    pl.semaphore_wait(barrier, 3)

    def chunk(k, _):
        wait(x_copies(k))

        @pl.when((k > 0) & (k + 1 < n_chunks))
        def _():
            start(x_copies(k + 1))

        def both(i, _):
            @pl.when((k > 0) & (i != 4) & (i != 8))
            def _():
                term_step(k - 1, i - i // 5)

            @pl.when((k == 0) & (i == n_gu - 3))
            def _():
                start(x_copies(1))
                wd_copy(0).start()

            @pl.when((k == 0) & (i == n_gu - 1))
            def _():
                wd_copy(1).start()

            hidden_step(k, i)
            return 0

        lax.fori_loop(0, n_gu, both, 0)

        return 0

    lax.fori_loop(0, n_chunks, chunk, 0)

    def term_only(j, _):
        term_step(n_chunks - 1, j)
        return 0

    lax.fori_loop(0, n_dn, term_only, 0)

    def last(n, _):
        tick(n)
        return 0

    lax.fori_loop(n_units - 1, n_units + L5, last, 0)
    half_y = y_hbm.at[pl.ds(0, y_hbm.shape[0] // 2)]
    remote(half_y, half_y, q_send, q_recv, sib).wait()


def solution(mesh):
    def step(x, w_gate, w_up, w_down):
        rows, depth = x.shape
        hidden = w_gate.shape[1]
        n_chunks, n_gu, n_dn = rows // M, hidden // TH, depth // W
        dma = pltpu.SemaphoreType.DMA
        y = pl.pallas_call(
            functools.partial(kernel, n_chunks, n_gu, n_dn),
            out_shape=jax.ShapeDtypeStruct((rows, depth), BF16),
            in_specs=[pl.BlockSpec(memory_space=pl.ANY)] * 4,
            out_specs=pl.BlockSpec(memory_space=pl.ANY),
            scratch_shapes=[
                pltpu.VMEM((2, M, depth), BF16),
                pltpu.VMEM((2, depth, 2 * TH), BF16),
                pltpu.VMEM((M, 2 * TH), F32),
                pltpu.VMEM((2, M, hidden), BF16),
                pltpu.VMEM((n_dn, hidden, W), BF16),
                pltpu.VMEM((RK, HALF, W), F32),
                pltpu.VMEM((RK, HALF, W), BF16),
                pltpu.VMEM((RK, HALF, W), BF16),
                pltpu.VMEM((4, QUARTER, W), F32),
                pltpu.VMEM((4, QUARTER, W), BF16),
                pltpu.VMEM((4, QUARTER, W), BF16),
                pltpu.VMEM((4, EIGHTH, W), F32),
                pltpu.VMEM((4, EIGHTH, W), BF16),
                pltpu.VMEM((4, EIGHTH, W), BF16),
                pltpu.VMEM((4, EIGHTH, W), BF16),
                dma((2, 2)), dma((2, 2, 2)), dma((n_dn,)),
                dma((RK,)), dma((RK,)),
                dma((4,)), dma((4,)),
                dma((4,)), dma((4,)),
                dma((4,)), dma((8,)), dma((8,)),
                dma, dma,
            ],
            compiler_params=pltpu.CompilerParams(
                collective_id=0, has_side_effects=True, vmem_limit_bytes=67043328
            ),
        )(x, w_gate, w_up, w_down)
        return y

    return jax.shard_map(
        step,
        mesh=mesh,
        in_specs=(P("dp", None), P(None, "tp"), P(None, "tp"), P("tp", None)),
        out_specs=P("dp", None),
        check_vma=False,
    )
```
